256 devices in a mesh: row: 8 (over y, core), col: 32 (over x, z).
Axes of the slice: x: 4, y: 4, z: 8, core: 2. Of those that a mesh axis runs over, the one named last changes fastest.
Arguments:
- inner_base: bfloat16 [4, 1, 2, 4096, 14336], P(None, None, None, 'row', 'col'), may hold values from -250 to 250
- inner_left: bfloat16 [4, 1, 2, 4096, 16], P(None, None, None, ('row', 'col')), may hold values from -6 to 6
- inner_right: bfloat16 [4, 1, 2, 16, 14336], P(None, None, None, 'row', 'col'), may hold values from -12 to 12
- inner_mag: float32 [4, 1, 2, 14336], P(None, None, None, 'col'), may hold values from 512 to 2048
- outer_base: bfloat16 [4, 1, 14336, 4096], P(None, None, 'row', 'col'), may hold values from -250 to 250
- outer_left: bfloat16 [4, 1, 14336, 16], P(None, None, ('row', 'col')), may hold values from -6 to 6
- outer_right: bfloat16 [4, 1, 16, 4096], P(None, None, 'row', 'col'), may hold values from -12 to 12
- outer_mag: float32 [4, 1, 4096], P(None, None, 'col'), may hold values from 1792 to 7168
Outputs:
- inner_merged: bfloat16 [4, 1, 2, 4096, 14336], P(None, None, None, 'row', 'col')
- outer_merged: bfloat16 [4, 1, 14336, 4096], P(None, None, 'row', 'col')
The draws below stay inside these ranges and needn't reach their ends.
All inputs are finite; a program needn't handle non-finite values.
Results may differ from the reference program's by a relative error of at most 0.001.
Values may be sent and summed in bfloat16 or wider, within the bound.
No kernel may reach another device: no remote copies, remote signals or barrier semaphores. Data moves between devices by JAX's collectives and lax.ppermute only.
A program may use at most 64 MiB of HBM per device.

```python
import math
import jax
import jax.numpy as jnp
from jax import lax

D = 4096
FF = 14336
RANK = 16
LAYERS = 4
EXPERTS = 1


def base_draw(key, extent):
    row_count = extent[-2]
    key_one, key_two = jax.random.split(key)
    scale_extent = extent[:-1] + (1,)
    jitter = jnp.clip(jax.random.normal(key_one, extent, jnp.float32), -6.0, 6.0)
    roughness = jnp.exp(jax.random.uniform(key_two, scale_extent, jnp.float32, 0.0, math.log(10.0)))
    growth = 2.0
    position = jnp.arange(row_count, dtype=jnp.float32) / max(row_count - 1, 1)
    rising = 1.0 + growth * position
    return (jitter * roughness * rising[:, None]).astype(jnp.bfloat16)


def draw_inner_base(key, part):
    return base_draw(jax.random.fold_in(key, 11), (LAYERS, EXPERTS, 2, D, FF))


def draw_outer_base(key, part):
    return base_draw(jax.random.fold_in(key, 23), (LAYERS, EXPERTS, FF, D))


def levels(rng, dims, pieces, least, top_value):
    level, own = 1.0, jax.random.fold_in(rng, 6)
    for dim, parts in pieces:
        steps = jnp.exp(jax.random.uniform(jax.random.fold_in(own, dim), (parts,), jnp.float32, least / len(pieces), top_value / len(pieces)))
        level = level * jnp.repeat(steps, dims[dim] // parts).reshape([-1 if axis == dim else 1 for axis in range(len(dims))])
    return level


def gaussian(key, dims, deviation, reach, pieces=(), kind=jnp.bfloat16):
    entries = deviation * jax.random.normal(key, dims, jnp.float32)
    if pieces:
        entries = entries * levels(key, dims, pieces, -0.22, 0.18)
    return jnp.clip(entries, -reach, reach).astype(kind)


def setup_inputs(seed: int = 0) -> dict:
    key_list = jax.random.split(jax.random.key(seed), 9)
    return {
        "inner_base": draw_inner_base(jax.random.fold_in(key_list[8], 71), 0),
        "inner_left": gaussian(key_list[1], (LAYERS, EXPERTS, 2, D, RANK), 1.0, 6.0, ((3, 256),)),
        "inner_right": gaussian(key_list[2], (LAYERS, EXPERTS, 2, RANK, FF), 2.0, 12.0, ((3, 8), (4, 32))),
        "inner_mag": jnp.clip(jnp.exp(math.log(2048.0) - 1.3862944 * jax.random.uniform(key_list[3], (LAYERS, EXPERTS, 2, FF), jnp.float32) ** levels(key_list[3], (LAYERS, EXPERTS, 2, FF), ((3, 32),), -0.2, 0.2)), 512.0, 2048.0),
        "outer_base": draw_outer_base(jax.random.fold_in(key_list[8], 71), 0),
        "outer_left": gaussian(key_list[5], (LAYERS, EXPERTS, FF, RANK), 1.0, 6.0, ((2, 256),)),
        "outer_right": gaussian(key_list[6], (LAYERS, EXPERTS, RANK, D), 2.0, 12.0, ((2, 8), (3, 32))),
        "outer_mag": jnp.clip(jnp.exp(math.log(7168.0) - 1.3862944 * jax.random.uniform(key_list[7], (LAYERS, EXPERTS, D), jnp.float32) ** levels(key_list[7], (LAYERS, EXPERTS, D), ((2, 32),), -0.2, 0.2)), 1792.0, 7168.0),
    }


epsilon = 1e-06

def merge_one(base, left, right, magnitude):
    delta = jnp.einsum('...ik,...kj->...ij', left.astype(jnp.float32), right.astype(jnp.float32))
    combined = base.astype(jnp.float32) + delta
    squares = lax.optimization_barrier(jnp.sum(combined * combined, axis=-2))
    factor = magnitude * lax.rsqrt(squares + epsilon)
    return (factor[..., None, :] * combined).astype(jnp.bfloat16)

def reference(inner_base, inner_left, inner_right, inner_mag, outer_base, outer_left, outer_right, outer_mag):
    inner_layers = []
    outer_layers = []
    for layer_index in range(LAYERS):
        inner_items = []
        outer_items = []
        for expert_index in range(EXPERTS):
            inner_items.append(merge_one(inner_base[layer_index, expert_index], inner_left[layer_index, expert_index], inner_right[layer_index, expert_index], inner_mag[layer_index, expert_index]))
            outer_items.append(merge_one(outer_base[layer_index, expert_index], outer_left[layer_index, expert_index], outer_right[layer_index, expert_index], outer_mag[layer_index, expert_index]))
        inner_layers.append(jnp.stack(inner_items))
        outer_layers.append(jnp.stack(outer_items))
    return (jnp.stack(inner_layers), jnp.stack(outer_layers))
```

```python
import jax
import jax.numpy as jnp
from jax import lax
from jax.experimental import pallas as pl
from jax.experimental.pallas import tpu as pltpu
from jax.sharding import PartitionSpec as P

epsilon = 1e-06
F32, BF16 = jnp.float32, jnp.bfloat16
MIB = 1 << 20


def iota(shape, dim):
    return lax.broadcasted_iota(jnp.int32, shape, dim)


def whole():
    return pl.BlockSpec(memory_space=pltpu.VMEM)


def params(mib):
    return pltpu.CompilerParams(vmem_limit_bytes=mib * MIB)


def dot(a, b, dims):
    return lax.dot_general(a, b, (dims, ((), ())), preferred_element_type=F32)


def pack_left_kernel(inner_ref, outer_ref, out_ref):
    k, lane = iota((16, 128), 0), iota((16, 128), 1)
    inner = jnp.zeros((16, 128), F32)
    for m in range(8):
        pick = (lane == 16 * (k // 2) + 2 * m + k % 2).astype(F32).astype(BF16)
        inner += dot(inner_ref[m], pick, ((1,), (0,)))
    k, lane = iota((16, 256), 0), iota((16, 256), 1)
    outer = jnp.zeros((56, 256), F32)
    for l in range(4):
        at = 8 * (k // 2) + 2 * l + k % 2
        pick = jnp.logical_or(lane == at, lane == at + 192).astype(F32).astype(BF16)
        outer += dot(outer_ref[l], pick, ((0,), (0,)))
    first = outer[0:32, 0:128]
    second = jnp.concatenate([outer[32:56, 128:256], jnp.zeros((8, 128), F32)], axis=0)
    block = jnp.concatenate([inner, first + second], axis=0).astype(BF16)
    for i in range(out_ref.shape[0]):
        out_ref[i] = block


def pack_right_kernel(inner_ref, outer_ref, out_ref):
    row, e = iota((16, 2), 0), iota((16, 2), 1)
    inner = jnp.zeros((16, 448), F32)
    for m in range(8):
        pick = (row == 2 * m + e).astype(F32).astype(BF16)
        inner += dot(pick, inner_ref[m], ((1,), (0,)))
    row, e = iota((8, 2), 0), iota((8, 2), 1)
    outer = jnp.zeros((8, 128), F32)
    for l in range(4):
        pick = (row == 2 * l + e).astype(F32).astype(BF16)
        outer += dot(pick, outer_ref[l], ((1,), (0,)))
    inner = jnp.concatenate([inner, jnp.zeros((16, 64), F32)], axis=1)
    outer = jnp.concatenate([outer, jnp.zeros((8, 384), F32)], axis=1)
    block = jnp.concatenate([inner, outer], axis=0).astype(BF16)
    for i in range(out_ref.shape[0]):
        out_ref[i] = block


def spread_right_kernel(right_ref, inner_ref, outer_ref):
    turned = right_ref[:, 0:16, :].reshape(128, 512).astype(F32).T[0:448, :]
    matrix = (iota((448, 128), 1) % 16) // 2
    for m in range(8):
        inner_ref[m] = jnp.where(matrix == m, turned, 0.0).astype(BF16)
    ranks = right_ref[:, 16:24, 0:128].astype(F32).reshape(64, 128)
    matrix = (iota((64, 128), 0) % 8) // 2
    zero = jnp.zeros((64, 128), F32)
    for l in range(4):
        one = jnp.where(matrix == l, ranks, 0.0)
        outer_ref[l, 0:64, :] = jnp.concatenate([one, zero], axis=1).astype(BF16)
        outer_ref[l, 64:128, :] = jnp.concatenate([zero, one], axis=1).astype(BF16)


def squares_kernel(
    left_ref, inner_right_ref, outer_right_ref, inner_ref, outer_ref, inner_full_ref, outer_full_ref, squares_ref
):
    left = left_ref[:, 0:16, :].reshape(512, 128)
    sums = []
    for m in range(8):
        full = inner_ref[m].astype(F32) + dot(inner_right_ref[m], left, ((1,), (1,)))
        inner_full_ref[m] = full
        square = full * full
        part = (square[:, 0:128] + square[:, 128:256]) + (square[:, 256:384] + square[:, 384:512])
        sums.append(jnp.sum(part.T, axis=0, keepdims=True))
    left = left_ref[:, 16:48, :].reshape(1024, 128)
    tails = []
    for l in range(4):
        delta = dot(left, outer_right_ref[l], ((1,), (0,)))
        total = jnp.zeros((8, 128), F32)
        for c in range(32):
            here = slice(56 * c, 56 * c + 56)
            two = jnp.concatenate([delta[32 * c : 32 * c + 32, 0:128], delta[32 * c : 32 * c + 24, 128:256]], axis=0)
            full = outer_ref[l, here, :].astype(F32) + two
            outer_full_ref[l, here, :] = full
            total += jnp.sum((full * full).reshape(7, 8, 128), axis=0)
        total = jnp.sum(total, axis=0, keepdims=True)
        tails += [total[:, 0:64], total[:, 64:128]]
    block = jnp.concatenate(
        [jnp.concatenate([s, t], axis=1) for s, t in zip(sums, tails)], axis=0
    )
    for i in range(squares_ref.shape[0]):
        squares_ref[i] = block


def scale_kernel(
    squares_ref, inner_mag_ref, outer_mag_ref, inner_full_ref, outer_full_ref, inner_out, outer_out, inner_buf, outer_buf, sems
):
    scale = lax.rsqrt(jnp.sum(squares_ref[...], axis=0) + epsilon)
    mags = jnp.concatenate([inner_mag_ref[i] for i in range(4)], axis=0)
    factor = (scale[:, 0:448] * mags).T
    copies = []
    for m in range(8):
        column = factor[:, m : m + 1]
        inner_buf[m] = (inner_full_ref[m] * column).astype(BF16)
        copies.append(pltpu.make_async_copy(inner_buf.at[m], inner_out.at[m], sems.at[m]))
        copies[-1].start()
        if m % 2:
            l = m // 2
            row = jnp.concatenate([scale[2 * l : 2 * l + 1, 448:512], scale[2 * l + 1 : 2 * l + 2, 448:512]], axis=1)
            row = row * outer_mag_ref[l]
            outer_buf[l] = (outer_full_ref[l] * row).astype(BF16)
            copies.append(pltpu.make_async_copy(outer_buf.at[l], outer_out.at[l], sems.at[8 + l]))
            copies[-1].start()
    for copy in copies:
        copy.wait()


def exchange(blocks, axis):
    return lax.all_to_all(blocks, axis, 0, 0, tiled=True)


def shards(
    inner_base, inner_left, inner_right, inner_mag, outer_base, outer_left, outer_right, outer_mag
):
    rows, cols = lax.axis_size("row"), lax.axis_size("col")
    inner_base = jnp.swapaxes(inner_base, 3, 4).reshape(8, 448, 512)
    outer_base = outer_base.reshape(4, 1792, 128)
    left = pl.pallas_call(
        pack_left_kernel,
        out_shape=pltpu.VMEM((cols, 48, 128), BF16),
        in_specs=[whole()] * 2,
        out_specs=whole(),
        compiler_params=params(4),
        name="pack_left",
    )(inner_left.reshape(8, 16, 16), jnp.swapaxes(outer_left, 2, 3).reshape(4, 16, 56))
    left = exchange(left, "col")
    right = pl.pallas_call(
        pack_right_kernel,
        out_shape=pltpu.VMEM((rows, 24, 512), BF16),
        in_specs=[whole()] * 2,
        out_specs=whole(),
        compiler_params=params(4),
        name="pack_right",
    )(inner_right.reshape(8, 2, 448), outer_right.reshape(4, 2, 128))
    right = exchange(right, "row")
    inner_ranks, outer_ranks = pl.pallas_call(
        spread_right_kernel,
        out_shape=(pltpu.VMEM((8, 448, 128), BF16), pltpu.VMEM((4, 128, 256), BF16)),
        in_specs=[whole()],
        out_specs=(whole(), whole()),
        compiler_params=params(4),
        name="spread_right",
    )(right)
    inner_full, outer_full, squares = pl.pallas_call(
        squares_kernel,
        out_shape=(
            pltpu.VMEM((8, 448, 512), F32),
            pltpu.VMEM((4, 1792, 128), F32),
            pltpu.VMEM((rows, 8, 512), F32),
        ),
        in_specs=[whole()] * 5,
        out_specs=(whole(),) * 3,
        compiler_params=params(12),
        name="squares",
    )(left, inner_ranks, outer_ranks, inner_base, outer_base)
    squares = exchange(squares, "row")
    inner_merged, outer_merged = pl.pallas_call(
        scale_kernel,
        out_shape=(
            jax.ShapeDtypeStruct((8, 448, 512), BF16),
            jax.ShapeDtypeStruct((4, 1792, 128), BF16),
        ),
        in_specs=[whole()] * 5,
        out_specs=(pl.BlockSpec(memory_space=pltpu.HBM),) * 2,
        scratch_shapes=[
            pltpu.VMEM((8, 448, 512), BF16),
            pltpu.VMEM((4, 1792, 128), BF16),
            pltpu.SemaphoreType.DMA((12,)),
        ],
        compiler_params=params(12),
        name="scale",
    )(squares, inner_mag.reshape(4, 2, 448), outer_mag, inner_full, outer_full)
    inner_merged = jnp.swapaxes(inner_merged.reshape(4, 1, 2, 448, 512), 3, 4)
    return inner_merged, outer_merged.reshape(4, 1, 1792, 128)


def solution(mesh):
    in_specs = (
        P(None, None, None, "row", "col"),
        P(None, None, None, ("row", "col"), None),
        P(None, None, None, "row", "col"),
        P(None, None, None, "col"),
        P(None, None, "row", "col"),
        P(None, None, ("row", "col"), None),
        P(None, None, "row", "col"),
        P(None, None, "col"),
    )
    out_specs = (P(None, None, None, "row", "col"), P(None, None, "row", "col"))
    return jax.shard_map(shards, mesh=mesh, in_specs=in_specs, out_specs=out_specs, check_vma=False)
```

```python
import jax
import jax.numpy as jnp
from jax import lax
from jax.experimental import pallas as pl
from jax.experimental.pallas import tpu as pltpu
from jax.sharding import PartitionSpec as P


epsilon = 1e-06
F32, BF16 = jnp.float32, jnp.bfloat16
MIB = 1 << 20
FAR = (3, 7, 5)
EARLY = 6


def iota(shape, dim):
    return lax.broadcasted_iota(jnp.int32, shape, dim)


def whole():
    return pl.BlockSpec(memory_space=pltpu.VMEM)


def in_hbm():
    return pl.BlockSpec(memory_space=pltpu.HBM)


def kept(value):
    return pltpu.with_memory_space_constraint(value, pltpu.HBM)


def params(mib):
    return pltpu.CompilerParams(vmem_limit_bytes=mib * MIB)


def fetch(pairs, sems):
    copies = [pltpu.make_async_copy(a, b, sems.at[i]) for i, (a, b) in enumerate(pairs)]
    for copy in copies:
        copy.start()
    for copy in copies:
        copy.wait()


def dot(a, b, dims):
    return lax.dot_general(a, b, (dims, ((), ())), preferred_element_type=F32)


def pack_kernel(
    inner_left_hbm, outer_left_hbm, inner_right_hbm, outer_right_hbm, left_out, right_out,
    inner_left_ref, outer_left_ref, inner_right_ref, outer_right_ref, sems
):
    fetch(
        [
            (inner_left_hbm, inner_left_ref),
            (outer_left_hbm, outer_left_ref),
            (inner_right_hbm, inner_right_ref),
            (outer_right_hbm, outer_right_ref),
        ],
        sems,
    )
    k, lane = iota((16, 128), 0), iota((16, 128), 1)
    inner = jnp.zeros((16, 128), F32)
    for m in range(8):
        pick = (lane == 16 * (k // 2) + 2 * m + k % 2).astype(F32).astype(BF16)
        inner += dot(inner_left_ref[m], pick, ((1,), (0,)))
    k, lane = iota((16, 256), 0), iota((16, 256), 1)
    outer = jnp.zeros((56, 256), F32)
    for l in range(4):
        at = 8 * (k // 2) + 2 * l + k % 2
        pick = jnp.logical_or(lane == at, lane == at + 192).astype(F32).astype(BF16)
        outer += dot(outer_left_ref[l], pick, ((0,), (0,)))
    first = outer[0:32, 0:128]
    second = jnp.concatenate([outer[32:56, 128:256], jnp.zeros((8, 128), F32)], axis=0)
    block = jnp.concatenate([inner, first + second], axis=0).astype(BF16)
    for i in range(left_out.shape[0]):
        left_out[i] = block
    row, e = iota((16, 2), 0), iota((16, 2), 1)
    inner = jnp.zeros((16, 448), F32)
    for m in range(8):
        pick = (row == 2 * m + e).astype(F32).astype(BF16)
        inner += dot(pick, inner_right_ref[m], ((1,), (0,)))
    row, e = iota((8, 2), 0), iota((8, 2), 1)
    outer = jnp.zeros((8, 128), F32)
    for l in range(4):
        pick = (row == 2 * l + e).astype(F32).astype(BF16)
        outer += dot(pick, outer_right_ref[l], ((1,), (0,)))
    inner = jnp.concatenate([inner, jnp.zeros((16, 64), F32)], axis=1)
    outer = jnp.concatenate([outer, jnp.zeros((8, 384), F32)], axis=1)
    right_out[...] = jnp.concatenate([inner, outer], axis=0).astype(BF16)


def gather_right_kernel(own_ref, one_ref, two_ref, three_ref, inner_ref, outer_ref, right_ref):
    me = lax.axis_index("row")
    for d, ref in zip((0, *FAR), (own_ref, one_ref, two_ref, three_ref)):
        for core in range(2):
            right_ref[me ^ (d ^ core)] = ref[core].astype(F32)
    inner_ref[...] = right_ref[:, 0:16, :].reshape(128, 512).T[0:448, :].astype(BF16)
    ranks = right_ref[:, 16:24, 0:128].reshape(64, 128)
    matrix = (iota((64, 128), 0) % 8) // 2
    zero = jnp.zeros((64, 128), F32)
    for l in range(4):
        one = jnp.where(matrix == l, ranks, 0.0)
        outer_ref[l, 0:64, :] = jnp.concatenate([one, zero], axis=1).astype(BF16)
        outer_ref[l, 64:128, :] = jnp.concatenate([zero, one], axis=1).astype(BF16)


def load_kernel(inner_hbm, inner_ref, sems):
    fetch([(inner_hbm.at[0:EARLY], inner_ref)], sems)


def squares_kernel(
    left_ref, inner_right_ref, outer_right_ref, early_ref, inner_hbm, outer_hbm,
    inner_full_ref, outer_full_ref, squares_ref, late_ref, outer_ref, sems
):
    def start_inner(i, carry):
        pltpu.make_async_copy(inner_hbm.at[EARLY + i], late_ref.at[i], sems.at[i]).start()
        return carry

    def start_outer(l, carry):
        pltpu.make_async_copy(outer_hbm.at[l], outer_ref.at[l], sems.at[8 - EARLY + l]).start()
        return carry

    lax.fori_loop(0, 8 - EARLY, start_inner, 0)
    lax.fori_loop(0, 4, start_outer, 0)
    left = left_ref[:, 0:16, :].reshape(512, 128)
    matrix = (iota((1, 128), 1) % 16) // 2
    sums = []
    for m in range(8):
        if m == EARLY:
            for i in range(8 - EARLY):
                pltpu.make_async_copy(inner_hbm.at[EARLY + i], late_ref.at[i], sems.at[i]).wait()
            for l in range(4):
                pltpu.make_async_copy(outer_hbm.at[l], outer_ref.at[l], sems.at[8 - EARLY + l]).wait()
        base = early_ref[m] if m < EARLY else late_ref[m - EARLY]
        right = inner_right_ref[...] * (matrix == m).astype(F32).astype(BF16)
        full = base.astype(F32) + dot(right, left, ((1,), (1,)))
        inner_full_ref[m] = full
        square = full * full
        part = (square[:, 0:128] + square[:, 128:256]) + (square[:, 256:384] + square[:, 384:512])
        sums.append(jnp.sum(part.T, axis=0, keepdims=True))
    left = left_ref[:, 16:48, :].reshape(1024, 128)
    tails = []
    for l in range(4):
        delta = dot(left, outer_right_ref[l], ((1,), (0,)))
        total = jnp.zeros((8, 128), F32)
        for c in range(32):
            here = slice(56 * c, 56 * c + 56)
            two = jnp.concatenate([delta[32 * c : 32 * c + 32, 0:128], delta[32 * c : 32 * c + 24, 128:256]], axis=0)
            full = outer_ref[l, here, :].astype(F32) + two
            outer_full_ref[l, here, :] = full
            total += jnp.sum((full * full).reshape(7, 8, 128), axis=0)
        total = jnp.sum(total, axis=0, keepdims=True)
        tails += [total[:, 0:64], total[:, 64:128]]
    squares_ref[...] = jnp.concatenate(
        [jnp.concatenate([s, t], axis=1) for s, t in zip(sums, tails)], axis=0
    )


def scale_kernel(
    own_ref, one_ref, two_ref, three_ref, inner_mag_ref, outer_mag_ref, inner_full_ref, outer_full_ref, inner_out, outer_out, inner_buf, outer_buf, sems
):
    scale = lax.rsqrt((own_ref[...] + one_ref[...]) + (two_ref[...] + three_ref[...]) + epsilon)
    mags = jnp.concatenate([inner_mag_ref[i] for i in range(4)], axis=0)
    factor = (scale[:, 0:448] * mags).T
    copies = []
    for m in range(8):
        column = factor[:, m : m + 1]
        inner_buf[m] = (inner_full_ref[m] * column).astype(BF16)
        copies.append(pltpu.make_async_copy(inner_buf.at[m], inner_out.at[m], sems.at[m]))
        copies[-1].start()
        if m % 2:
            l = m // 2
            row = jnp.concatenate([scale[2 * l : 2 * l + 1, 448:512], scale[2 * l + 1 : 2 * l + 2, 448:512]], axis=1)
            row = row * outer_mag_ref[l]
            outer_buf[l] = (outer_full_ref[l] * row).astype(BF16)
            copies.append(pltpu.make_async_copy(outer_buf.at[l], outer_out.at[l], sems.at[8 + l]))
            copies[-1].start()
    for copy in copies:
        copy.wait()


def swapped(value, d):
    return lax.ppermute(value, "row", [(i, i ^ d) for i in range(lax.axis_size("row"))])


def shards(
    inner_base, inner_left, inner_right, inner_mag, outer_base, outer_left, outer_right, outer_mag
):
    cols = lax.axis_size("col")
    inner_base = jnp.swapaxes(inner_base, 3, 4).reshape(8, 448, 512)
    outer_base = outer_base.reshape(4, 1792, 128)
    left, right = pl.pallas_call(
        pack_kernel,
        out_shape=(pltpu.VMEM((cols, 48, 128), BF16), pltpu.VMEM((24, 512), BF16)),
        in_specs=[in_hbm()] * 4,
        out_specs=(whole(),) * 2,
        scratch_shapes=[
            pltpu.VMEM((8, 16, 16), BF16),
            pltpu.VMEM((4, 16, 56), BF16),
            pltpu.VMEM((8, 2, 448), BF16),
            pltpu.VMEM((4, 2, 128), BF16),
            pltpu.SemaphoreType.DMA((4,)),
        ],
        compiler_params=params(4),
        name="pack",
    )(
        kept(inner_left.reshape(8, 16, 16)),
        kept(jnp.swapaxes(outer_left, 2, 3).reshape(4, 16, 56)),
        kept(inner_right.reshape(8, 2, 448)),
        kept(outer_right.reshape(4, 2, 128)),
    )
    partner = swapped(right, 1)
    left = lax.all_to_all(left, "col", 0, 0, tiled=True)
    right = jnp.stack([right, partner])
    far = [swapped(right, d) for d in FAR]
    early = pl.pallas_call(
        load_kernel,
        out_shape=pltpu.VMEM((EARLY, 448, 512), BF16),
        in_specs=[in_hbm()],
        out_specs=whole(),
        scratch_shapes=[pltpu.SemaphoreType.DMA((1,))],
        compiler_params=params(4),
        name="load",
    )(kept(inner_base))
    inner_ranks, outer_ranks = pl.pallas_call(
        gather_right_kernel,
        out_shape=(pltpu.VMEM((448, 128), BF16), pltpu.VMEM((4, 128, 256), BF16)),
        in_specs=[whole()] * 4,
        out_specs=(whole(), whole()),
        scratch_shapes=[pltpu.VMEM((8, 24, 512), F32)],
        compiler_params=params(4),
        name="gather_right",
    )(right, *far)
    inner_full, outer_full, squares = pl.pallas_call(
        squares_kernel,
        out_shape=(
            pltpu.VMEM((8, 448, 512), F32),
            pltpu.VMEM((4, 1792, 128), F32),
            pltpu.VMEM((8, 512), F32),
        ),
        in_specs=[whole()] * 4 + [in_hbm()] * 2,
        out_specs=(whole(),) * 3,
        scratch_shapes=[
            pltpu.VMEM((8 - EARLY, 448, 512), BF16),
            pltpu.VMEM((4, 1792, 128), BF16),
            pltpu.SemaphoreType.DMA((12 - EARLY,)),
        ],
        compiler_params=params(12),
        name="squares",
    )(left, inner_ranks, outer_ranks, early, kept(inner_base), kept(outer_base))
    squares = squares + swapped(squares, 1)
    far = [swapped(squares, d) for d in FAR]
    inner_merged, outer_merged = pl.pallas_call(
        scale_kernel,
        out_shape=(
            jax.ShapeDtypeStruct((8, 448, 512), BF16),
            jax.ShapeDtypeStruct((4, 1792, 128), BF16),
        ),
        in_specs=[whole()] * 8,
        out_specs=(in_hbm(),) * 2,
        scratch_shapes=[
            pltpu.VMEM((8, 448, 512), BF16),
            pltpu.VMEM((4, 1792, 128), BF16),
            pltpu.SemaphoreType.DMA((12,)),
        ],
        compiler_params=params(12),
        name="scale",
    )(squares, *far, inner_mag.reshape(4, 2, 448), outer_mag, inner_full, outer_full)
    inner_merged = jnp.swapaxes(inner_merged.reshape(4, 1, 2, 448, 512), 3, 4)
    return inner_merged, outer_merged.reshape(4, 1, 1792, 128)


def solution(mesh):
    in_specs = (
        P(None, None, None, "row", "col"),
        P(None, None, None, ("row", "col"), None),
        P(None, None, None, "row", "col"),
        P(None, None, None, "col"),
        P(None, None, "row", "col"),
        P(None, None, ("row", "col"), None),
        P(None, None, "row", "col"),
        P(None, None, "col"),
    )
    out_specs = (P(None, None, None, "row", "col"), P(None, None, "row", "col"))
    return jax.shard_map(shards, mesh=mesh, in_specs=in_specs, out_specs=out_specs, check_vma=False)
```

```python
import jax
import jax.numpy as jnp
from jax import lax
from jax.experimental import pallas as pl
from jax.experimental.pallas import tpu as pltpu
from jax.sharding import PartitionSpec as P


epsilon = 1e-06
F32, BF16 = jnp.float32, jnp.bfloat16
MIB = 1 << 20
FAR = (3, 7, 5)
EARLY = 6


def iota(shape, dim):
    return lax.broadcasted_iota(jnp.int32, shape, dim)


def whole():
    return pl.BlockSpec(memory_space=pltpu.VMEM)


def in_hbm():
    return pl.BlockSpec(memory_space=pltpu.HBM)


def kept(value):
    return pltpu.with_memory_space_constraint(value, pltpu.HBM)


def params(mib):
    return pltpu.CompilerParams(vmem_limit_bytes=mib * MIB)


def fetch(pairs, sems):
    copies = [pltpu.make_async_copy(a, b, sems.at[i]) for i, (a, b) in enumerate(pairs)]
    for copy in copies:
        copy.start()
    for copy in copies:
        copy.wait()


def dot(a, b, dims):
    return lax.dot_general(a, b, (dims, ((), ())), preferred_element_type=F32)


def pack_kernel(
    inner_left_hbm, outer_left_hbm, inner_right_hbm, outer_right_hbm, left_out, right_out,
    inner_left_ref, outer_left_ref, inner_right_ref, outer_right_ref, left_ref, sems
):
    fetch(
        [
            (inner_left_hbm, inner_left_ref),
            (outer_left_hbm, outer_left_ref),
            (inner_right_hbm, inner_right_ref),
            (outer_right_hbm, outer_right_ref),
        ],
        sems,
    )
    k, lane = iota((16, 128), 0), iota((16, 128), 1)
    inner = jnp.zeros((16, 128), F32)
    for m in range(8):
        pick = (lane == 16 * (k // 2) + 2 * m + k % 2).astype(F32).astype(BF16)
        inner += dot(inner_left_ref[m], pick, ((1,), (0,)))
    k, lane = iota((16, 256), 0), iota((16, 256), 1)
    outer = jnp.zeros((56, 256), F32)
    for l in range(4):
        at = 8 * (k // 2) + 2 * l + k % 2
        pick = jnp.logical_or(lane == at, lane == at + 192).astype(F32).astype(BF16)
        outer += dot(outer_left_ref[l], pick, ((0,), (0,)))
    first = outer[0:32, 0:128]
    second = jnp.concatenate([outer[32:56, 128:256], jnp.zeros((8, 128), F32)], axis=0)
    block = jnp.concatenate([inner, first + second], axis=0).astype(BF16)
    for i in range(left_ref.shape[0]):
        left_ref[i] = block
    sent = pltpu.make_async_copy(left_ref, left_out, sems.at[4])
    sent.start()
    row, e = iota((16, 2), 0), iota((16, 2), 1)
    inner = jnp.zeros((16, 448), F32)
    for m in range(8):
        pick = (row == 2 * m + e).astype(F32).astype(BF16)
        inner += dot(pick, inner_right_ref[m], ((1,), (0,)))
    row, e = iota((8, 2), 0), iota((8, 2), 1)
    outer = jnp.zeros((8, 128), F32)
    for l in range(4):
        pick = (row == 2 * l + e).astype(F32).astype(BF16)
        outer += dot(pick, outer_right_ref[l], ((1,), (0,)))
    outer = jnp.concatenate([outer[:, 0:64], outer[:, 64:128]], axis=0)
    right_out[...] = jnp.concatenate([inner, outer], axis=1).astype(BF16)
    sent.wait()


def gather_right_kernel(own_ref, one_ref, two_ref, three_ref, inner_ref, outer_ref, right_ref):
    me = lax.axis_index("row")
    for d, ref in zip((0, *FAR), (own_ref, one_ref, two_ref, three_ref)):
        for core in range(2):
            right_ref[me ^ (d ^ core)] = ref[core].astype(F32)
    inner_ref[...] = right_ref[...].reshape(128, 512).T[0:448, :].astype(BF16)
    ranks = jnp.concatenate([right_ref[:, 0:8, 448:512], right_ref[:, 8:16, 448:512]], axis=2).reshape(64, 128)
    matrix = (iota((64, 128), 0) % 8) // 2
    zero = jnp.zeros((64, 128), F32)
    for l in range(4):
        one = jnp.where(matrix == l, ranks, 0.0)
        outer_ref[l, 0:64, :] = jnp.concatenate([one, zero], axis=1).astype(BF16)
        outer_ref[l, 64:128, :] = jnp.concatenate([zero, one], axis=1).astype(BF16)


def load_kernel(inner_hbm, inner_ref, sems):
    fetch([(inner_hbm.at[0:EARLY], inner_ref)], sems)


def squares_kernel(
    left_ref, inner_right_ref, outer_right_ref, early_ref, inner_hbm, outer_hbm,
    inner_full_ref, outer_full_ref, squares_ref, late_ref, outer_ref, sems
):
    def start_inner(i, carry):
        pltpu.make_async_copy(inner_hbm.at[EARLY + i], late_ref.at[i], sems.at[i]).start()
        return carry

    def start_outer(l, carry):
        pltpu.make_async_copy(outer_hbm.at[l], outer_ref.at[l], sems.at[8 - EARLY + l]).start()
        return carry

    lax.fori_loop(0, 8 - EARLY, start_inner, 0)
    left = left_ref[:, 0:16, :].reshape(512, 128)
    matrix = (iota((1, 128), 1) % 16) // 2
    sums = []
    for m in range(8):
        if m == 1:
            lax.fori_loop(0, 4, start_outer, 0)
        if m == EARLY:
            for i in range(8 - EARLY):
                pltpu.make_async_copy(inner_hbm.at[EARLY + i], late_ref.at[i], sems.at[i]).wait()
        base = early_ref[m] if m < EARLY else late_ref[m - EARLY]
        right = inner_right_ref[...] * (matrix == m).astype(F32).astype(BF16)
        full = base.astype(F32) + dot(right, left, ((1,), (1,)))
        inner_full_ref[m] = full
        square = full * full
        part = (square[:, 0:128] + square[:, 128:256]) + (square[:, 256:384] + square[:, 384:512])
        sums.append(jnp.sum(part.T, axis=0, keepdims=True))
    left = left_ref[:, 16:48, :].reshape(1024, 128)
    tails = []
    for l in range(4):
        pltpu.make_async_copy(outer_hbm.at[l], outer_ref.at[l], sems.at[8 - EARLY + l]).wait()
    for l in range(4):
        delta = dot(left, outer_right_ref[l], ((1,), (0,)))
        total = jnp.zeros((8, 128), F32)
        for c in range(32):
            here = slice(56 * c, 56 * c + 56)
            two = jnp.concatenate([delta[32 * c : 32 * c + 32, 0:128], delta[32 * c : 32 * c + 24, 128:256]], axis=0)
            full = outer_ref[l, here, :].astype(F32) + two
            outer_full_ref[l, here, :] = full
            total += jnp.sum((full * full).reshape(7, 8, 128), axis=0)
        total = jnp.sum(total, axis=0, keepdims=True)
        tails += [total[:, 0:64], total[:, 64:128]]
    squares_ref[...] = jnp.concatenate(
        [jnp.concatenate([s, t], axis=1) for s, t in zip(sums, tails)], axis=0
    )


def scale_kernel(
    own_ref, one_ref, two_ref, three_ref, inner_mag_ref, outer_mag_ref, inner_full_ref, outer_full_ref, inner_out, outer_out, inner_buf, outer_buf, sems
):
    here = lax.axis_index("row")
    scale = lax.rsqrt((own_ref[...] + one_ref[...]) + (two_ref[...] + three_ref[...]) + epsilon)
    mags = jnp.concatenate([inner_mag_ref[i] for i in range(4)], axis=0)
    factor = (scale[:, 0:448] * mags).T

    def sent_outer(l):
        return pltpu.make_async_copy(outer_buf.at[l], outer_out.at[l], sems.at[8 + l])

    def sent_inner(m):
        return pltpu.make_async_copy(inner_buf.at[m], inner_out.at[m], sems.at[m])

    for l in range(4):
        row = jnp.concatenate([scale[2 * l : 2 * l + 1, 448:512], scale[2 * l + 1 : 2 * l + 2, 448:512]], axis=1)
        row = row * outer_mag_ref[l]

        @pl.when(here >= 0)
        def _():
            outer_buf[l] = (outer_full_ref[l] * row).astype(BF16)
            sent_outer(l).start()

    for m in range(8):
        column = factor[:, m : m + 1]

        @pl.when(here >= 0)
        def _():
            inner_buf[m] = (inner_full_ref[m] * column).astype(BF16)
            sent_inner(m).start()

    for l in range(4):
        sent_outer(l).wait()
    for m in range(8):
        sent_inner(m).wait()


def swapped(value, d):
    return lax.ppermute(value, "row", [(i, i ^ d) for i in range(lax.axis_size("row"))])


def shards(
    inner_base, inner_left, inner_right, inner_mag, outer_base, outer_left, outer_right, outer_mag
):
    cols = lax.axis_size("col")
    inner_base = jnp.swapaxes(inner_base, 3, 4).reshape(8, 448, 512)
    outer_base = outer_base.reshape(4, 1792, 128)
    left, right = pl.pallas_call(
        pack_kernel,
        out_shape=(jax.ShapeDtypeStruct((cols, 48, 128), BF16), pltpu.VMEM((16, 512), BF16)),
        in_specs=[in_hbm()] * 4,
        out_specs=(in_hbm(), whole()),
        scratch_shapes=[
            pltpu.VMEM((8, 16, 16), BF16),
            pltpu.VMEM((4, 16, 56), BF16),
            pltpu.VMEM((8, 2, 448), BF16),
            pltpu.VMEM((4, 2, 128), BF16),
            pltpu.VMEM((cols, 48, 128), BF16),
            pltpu.SemaphoreType.DMA((5,)),
        ],
        compiler_params=params(4),
        name="pack",
    )(
        kept(inner_left.reshape(8, 16, 16)),
        kept(jnp.swapaxes(outer_left, 2, 3).reshape(4, 16, 56)),
        kept(inner_right.reshape(8, 2, 448)),
        kept(outer_right.reshape(4, 2, 128)),
    )
    partner = swapped(right, 1)
    left = lax.all_to_all(left, "col", 0, 0, tiled=True)
    right = jnp.stack([right, partner])
    far = [swapped(right, d) for d in FAR]
    early = pl.pallas_call(
        load_kernel,
        out_shape=pltpu.VMEM((EARLY, 448, 512), BF16),
        in_specs=[in_hbm()],
        out_specs=whole(),
        scratch_shapes=[pltpu.SemaphoreType.DMA((1,))],
        compiler_params=params(4),
        name="load",
    )(kept(inner_base))
    inner_ranks, outer_ranks = pl.pallas_call(
        gather_right_kernel,
        out_shape=(pltpu.VMEM((448, 128), BF16), pltpu.VMEM((4, 128, 256), BF16)),
        in_specs=[whole()] * 4,
        out_specs=(whole(), whole()),
        scratch_shapes=[pltpu.VMEM((8, 16, 512), F32)],
        compiler_params=params(4),
        name="gather_right",
    )(right, *far)
    inner_full, outer_full, squares = pl.pallas_call(
        squares_kernel,
        out_shape=(
            pltpu.VMEM((8, 448, 512), F32),
            pltpu.VMEM((4, 1792, 128), F32),
            pltpu.VMEM((8, 512), F32),
        ),
        in_specs=[whole()] * 4 + [in_hbm()] * 2,
        out_specs=(whole(),) * 3,
        scratch_shapes=[
            pltpu.VMEM((8 - EARLY, 448, 512), BF16),
            pltpu.VMEM((4, 1792, 128), BF16),
            pltpu.SemaphoreType.DMA((12 - EARLY,)),
        ],
        compiler_params=params(12),
        name="squares",
    )(left, inner_ranks, outer_ranks, early, kept(inner_base), kept(outer_base))
    squares = squares + swapped(squares, 1)
    far = [swapped(squares, d) for d in FAR]
    inner_merged, outer_merged = pl.pallas_call(
        scale_kernel,
        out_shape=(
            jax.ShapeDtypeStruct((8, 448, 512), BF16),
            jax.ShapeDtypeStruct((4, 1792, 128), BF16),
        ),
        in_specs=[whole()] * 8,
        out_specs=(in_hbm(),) * 2,
        scratch_shapes=[
            pltpu.VMEM((8, 448, 512), BF16),
            pltpu.VMEM((4, 1792, 128), BF16),
            pltpu.SemaphoreType.DMA((12,)),
        ],
        compiler_params=params(12),
        name="scale",
    )(squares, *far, inner_mag.reshape(4, 2, 448), outer_mag, inner_full, outer_full)
    inner_merged = jnp.swapaxes(inner_merged.reshape(4, 1, 2, 448, 512), 3, 4)
    return inner_merged, outer_merged.reshape(4, 1, 1792, 128)


def solution(mesh):
    in_specs = (
        P(None, None, None, "row", "col"),
        P(None, None, None, ("row", "col"), None),
        P(None, None, None, "row", "col"),
        P(None, None, None, "col"),
        P(None, None, "row", "col"),
        P(None, None, ("row", "col"), None),
        P(None, None, "row", "col"),
        P(None, None, "col"),
    )
    out_specs = (P(None, None, None, "row", "col"), P(None, None, "row", "col"))
    return jax.shard_map(shards, mesh=mesh, in_specs=in_specs, out_specs=out_specs, check_vma=False)
```

```python
import jax
import jax.numpy as jnp
from jax import lax
from jax.experimental import pallas as pl
from jax.experimental.pallas import tpu as pltpu
from jax.sharding import PartitionSpec as P


epsilon = 1e-06
F32, BF16 = jnp.float32, jnp.bfloat16
MIB = 1 << 20
FAR = (3, 7, 5)
EARLY = 6


def iota(shape, dim):
    return lax.broadcasted_iota(jnp.int32, shape, dim)


def whole():
    return pl.BlockSpec(memory_space=pltpu.VMEM)


def in_hbm():
    return pl.BlockSpec(memory_space=pltpu.HBM)


def kept(value):
    return pltpu.with_memory_space_constraint(value, pltpu.HBM)


def params(mib):
    return pltpu.CompilerParams(vmem_limit_bytes=mib * MIB)


def fetch(pairs, sems):
    copies = [pltpu.make_async_copy(a, b, sems.at[i]) for i, (a, b) in enumerate(pairs)]
    for copy in copies:
        copy.start()
    for copy in copies:
        copy.wait()


def dot(a, b, dims):
    return lax.dot_general(a, b, (dims, ((), ())), preferred_element_type=F32)


def pack_kernel(
    inner_left_hbm, outer_left_hbm, inner_right_hbm, outer_right_hbm, left_out, right_out,
    inner_left_ref, outer_left_ref, inner_right_ref, outer_right_ref, left_ref, sems
):
    fetch(
        [
            (inner_left_hbm, inner_left_ref),
            (outer_left_hbm, outer_left_ref),
            (inner_right_hbm, inner_right_ref),
            (outer_right_hbm, outer_right_ref),
        ],
        sems,
    )
    k, lane = iota((16, 128), 0), iota((16, 128), 1)
    inner = jnp.zeros((16, 128), F32)
    for m in range(8):
        pick = (lane == 16 * (k // 2) + 2 * m + k % 2).astype(F32).astype(BF16)
        inner += dot(inner_left_ref[m], pick, ((1,), (0,)))
    k, lane = iota((16, 256), 0), iota((16, 256), 1)
    outer = jnp.zeros((56, 256), F32)
    for l in range(4):
        at = 8 * (k // 2) + 2 * l + k % 2
        pick = jnp.logical_or(lane == at, lane == at + 192).astype(F32).astype(BF16)
        outer += dot(outer_left_ref[l], pick, ((0,), (0,)))
    first, second = outer[:, 0:128], outer[:, 128:256]
    block = jnp.concatenate([inner, first[0:24] + second[24:48], first[48:52] + second[52:56]], axis=0)
    for i in range(left_ref.shape[0]):
        left_ref[i] = block.reshape(11, 4, 128).astype(BF16)
    sent = pltpu.make_async_copy(left_ref, left_out, sems.at[4])
    sent.start()
    row, e = iota((16, 2), 0), iota((16, 2), 1)
    inner = jnp.zeros((16, 448), F32)
    for m in range(8):
        pick = (row == 2 * m + e).astype(F32).astype(BF16)
        inner += dot(pick, inner_right_ref[m], ((1,), (0,)))
    row, e = iota((8, 2), 0), iota((8, 2), 1)
    outer = jnp.zeros((8, 128), F32)
    for l in range(4):
        pick = (row == 2 * l + e).astype(F32).astype(BF16)
        outer += dot(pick, outer_right_ref[l], ((1,), (0,)))
    outer = jnp.concatenate([outer[:, 0:64], outer[:, 64:128]], axis=0)
    right_out[...] = jnp.concatenate([inner, outer], axis=1).astype(BF16)
    sent.wait()


def gather_right_kernel(own_ref, one_ref, two_ref, three_ref, inner_ref, outer_ref, right_ref):
    me = lax.axis_index("row")
    for d, ref in zip((0, *FAR), (own_ref, one_ref, two_ref, three_ref)):
        for core in range(2):
            right_ref[me ^ (d ^ core)] = ref[core].astype(F32)
    inner_ref[...] = right_ref[...].reshape(128, 512).T[0:448, :].astype(BF16)
    ranks = jnp.concatenate([right_ref[:, 0:8, 448:512], right_ref[:, 8:16, 448:512]], axis=2).reshape(64, 128)
    matrix = (iota((64, 128), 0) % 8) // 2
    zero = jnp.zeros((64, 128), F32)
    for l in range(4):
        one = jnp.where(matrix == l, ranks, 0.0)
        outer_ref[l, 0:64, :] = jnp.concatenate([one, zero], axis=1).astype(BF16)
        outer_ref[l, 64:128, :] = jnp.concatenate([zero, one], axis=1).astype(BF16)


def load_kernel(inner_hbm, inner_ref, sems):
    fetch([(inner_hbm.at[0:EARLY], inner_ref)], sems)


def squares_kernel(
    left_ref, inner_right_ref, outer_right_ref, early_ref, inner_hbm, outer_hbm,
    inner_full_ref, outer_full_ref, squares_ref, late_ref, outer_ref, sems
):
    def start_inner(i, carry):
        pltpu.make_async_copy(inner_hbm.at[EARLY + i], late_ref.at[i], sems.at[i]).start()
        return carry

    def start_outer(l, carry):
        pltpu.make_async_copy(outer_hbm.at[l], outer_ref.at[l], sems.at[8 - EARLY + l]).start()
        return carry

    lax.fori_loop(0, 8 - EARLY, start_inner, 0)
    lax.fori_loop(0, 4, start_outer, 0)
    left = left_ref[:, 0:4].astype(F32).reshape(512, 128).astype(BF16)
    matrix = (iota((1, 128), 1) % 16) // 2
    sums = []
    for m in range(8):
        if m == EARLY:
            for i in range(8 - EARLY):
                pltpu.make_async_copy(inner_hbm.at[EARLY + i], late_ref.at[i], sems.at[i]).wait()
        base = early_ref[m] if m < EARLY else late_ref[m - EARLY]
        right = inner_right_ref[...] * (matrix == m).astype(F32).astype(BF16)
        full = base.astype(F32) + dot(right, left, ((1,), (1,)))
        inner_full_ref[m] = full
        square = full * full
        part = (square[:, 0:128] + square[:, 128:256]) + (square[:, 256:384] + square[:, 384:512])
        sums.append(jnp.sum(part.T, axis=0, keepdims=True))
    left = jnp.concatenate([left_ref[:, 4:11], left_ref[:, 10:11]], axis=1).astype(F32)
    left = left.reshape(1024, 128).astype(BF16)
    upper = iota((8, 128), 0) < 4
    tails = []
    for l in range(4):
        pltpu.make_async_copy(outer_hbm.at[l], outer_ref.at[l], sems.at[8 - EARLY + l]).wait()
    for l in range(4):
        delta = dot(left, outer_right_ref[l], ((1,), (0,)))
        total = jnp.zeros((8, 128), F32)
        for c in range(32):
            here = slice(56 * c, 56 * c + 56)
            a, b = delta[32 * c : 32 * c + 32, 0:128], delta[32 * c : 32 * c + 32, 128:256]
            two = jnp.concatenate([a[0:24], b[0:24], jnp.where(upper, a[24:32], b[24:32])], axis=0)
            full = outer_ref[l, here, :].astype(F32) + two
            outer_full_ref[l, here, :] = full
            total += jnp.sum((full * full).reshape(7, 8, 128), axis=0)
        total = jnp.sum(total, axis=0, keepdims=True)
        tails += [total[:, 0:64], total[:, 64:128]]
    squares_ref[...] = jnp.concatenate(
        [jnp.concatenate([s, t], axis=1) for s, t in zip(sums, tails)], axis=0
    )


def scale_kernel(
    own_ref, one_ref, two_ref, three_ref, inner_mag_ref, outer_mag_ref, inner_full_ref, outer_full_ref, inner_out, outer_out, inner_buf, outer_buf, sems
):
    here = lax.axis_index("row")
    scale = lax.rsqrt((own_ref[...] + one_ref[...]) + (two_ref[...] + three_ref[...]) + epsilon)
    mags = jnp.concatenate([inner_mag_ref[i] for i in range(4)], axis=0)
    factor = (scale[:, 0:448] * mags).T

    def sent_outer(l):
        return pltpu.make_async_copy(outer_buf.at[l], outer_out.at[l], sems.at[8 + l])

    def sent_inner(m):
        return pltpu.make_async_copy(inner_buf.at[m], inner_out.at[m], sems.at[m])

    for l in range(4):
        row = jnp.concatenate([scale[2 * l : 2 * l + 1, 448:512], scale[2 * l + 1 : 2 * l + 2, 448:512]], axis=1)
        row = row * outer_mag_ref[l]

        @pl.when(here >= 0)
        def _():
            outer_buf[l] = (outer_full_ref[l] * row).astype(BF16)
            sent_outer(l).start()

    for m in range(8):
        column = factor[:, m : m + 1]

        @pl.when(here >= 0)
        def _():
            inner_buf[m] = (inner_full_ref[m] * column).astype(BF16)
            sent_inner(m).start()

    for l in range(4):
        sent_outer(l).wait()
    for m in range(8):
        sent_inner(m).wait()


def swapped(value, d):
    return lax.ppermute(value, "row", [(i, i ^ d) for i in range(lax.axis_size("row"))])


def shards(
    inner_base, inner_left, inner_right, inner_mag, outer_base, outer_left, outer_right, outer_mag
):
    cols = lax.axis_size("col")
    inner_base = jnp.swapaxes(inner_base, 3, 4).reshape(8, 448, 512)
    outer_base = outer_base.reshape(4, 1792, 128)
    left, right = pl.pallas_call(
        pack_kernel,
        out_shape=(jax.ShapeDtypeStruct((cols, 11, 4, 128), BF16), pltpu.VMEM((16, 512), BF16)),
        in_specs=[in_hbm()] * 4,
        out_specs=(in_hbm(), whole()),
        scratch_shapes=[
            pltpu.VMEM((8, 16, 16), BF16),
            pltpu.VMEM((4, 16, 56), BF16),
            pltpu.VMEM((8, 2, 448), BF16),
            pltpu.VMEM((4, 2, 128), BF16),
            pltpu.VMEM((cols, 11, 4, 128), BF16),
            pltpu.SemaphoreType.DMA((5,)),
        ],
        compiler_params=params(4),
        name="pack",
    )(
        kept(inner_left.reshape(8, 16, 16)),
        kept(jnp.swapaxes(outer_left, 2, 3).reshape(4, 16, 56)),
        kept(inner_right.reshape(8, 2, 448)),
        kept(outer_right.reshape(4, 2, 128)),
    )
    partner = swapped(right, 1)
    left = lax.all_to_all(left, "col", 0, 0, tiled=True)
    right = jnp.stack([right, partner])
    far = [swapped(right, d) for d in FAR]
    early = pl.pallas_call(
        load_kernel,
        out_shape=pltpu.VMEM((EARLY, 448, 512), BF16),
        in_specs=[in_hbm()],
        out_specs=whole(),
        scratch_shapes=[pltpu.SemaphoreType.DMA((1,))],
        compiler_params=params(4),
        name="load",
    )(kept(inner_base))
    inner_ranks, outer_ranks = pl.pallas_call(
        gather_right_kernel,
        out_shape=(pltpu.VMEM((448, 128), BF16), pltpu.VMEM((4, 128, 256), BF16)),
        in_specs=[whole()] * 4,
        out_specs=(whole(), whole()),
        scratch_shapes=[pltpu.VMEM((8, 16, 512), F32)],
        compiler_params=params(4),
        name="gather_right",
    )(right, *far)
    inner_full, outer_full, squares = pl.pallas_call(
        squares_kernel,
        out_shape=(
            pltpu.VMEM((8, 448, 512), F32),
            pltpu.VMEM((4, 1792, 128), F32),
            pltpu.VMEM((8, 512), F32),
        ),
        in_specs=[whole()] * 4 + [in_hbm()] * 2,
        out_specs=(whole(),) * 3,
        scratch_shapes=[
            pltpu.VMEM((8 - EARLY, 448, 512), BF16),
            pltpu.VMEM((4, 1792, 128), BF16),
            pltpu.SemaphoreType.DMA((12 - EARLY,)),
        ],
        compiler_params=params(12),
        name="squares",
    )(left, inner_ranks, outer_ranks, early, kept(inner_base), kept(outer_base))
    squares = squares + swapped(squares, 1)
    far = [swapped(squares, d) for d in FAR]
    inner_merged, outer_merged = pl.pallas_call(
        scale_kernel,
        out_shape=(
            jax.ShapeDtypeStruct((8, 448, 512), BF16),
            jax.ShapeDtypeStruct((4, 1792, 128), BF16),
        ),
        in_specs=[whole()] * 8,
        out_specs=(in_hbm(),) * 2,
        scratch_shapes=[
            pltpu.VMEM((8, 448, 512), BF16),
            pltpu.VMEM((4, 1792, 128), BF16),
            pltpu.SemaphoreType.DMA((12,)),
        ],
        compiler_params=params(12),
        name="scale",
    )(squares, *far, inner_mag.reshape(4, 2, 448), outer_mag, inner_full, outer_full)
    inner_merged = jnp.swapaxes(inner_merged.reshape(4, 1, 2, 448, 512), 3, 4)
    return inner_merged, outer_merged.reshape(4, 1, 1792, 128)


def solution(mesh):
    in_specs = (
        P(None, None, None, "row", "col"),
        P(None, None, None, ("row", "col"), None),
        P(None, None, None, "row", "col"),
        P(None, None, None, "col"),
        P(None, None, "row", "col"),
        P(None, None, ("row", "col"), None),
        P(None, None, "row", "col"),
        P(None, None, "col"),
    )
    out_specs = (P(None, None, None, "row", "col"), P(None, None, "row", "col"))
    return jax.shard_map(shards, mesh=mesh, in_specs=in_specs, out_specs=out_specs, check_vma=False)
```

```python
import jax
import jax.numpy as jnp
from jax import lax
from jax.experimental import pallas as pl
from jax.experimental.pallas import tpu as pltpu
from jax.sharding import PartitionSpec as P


epsilon = 1e-06
F32, BF16 = jnp.float32, jnp.bfloat16
MIB = 1 << 20
FAR = (3, 7, 5)
EARLY = 6


def iota(shape, dim):
    return lax.broadcasted_iota(jnp.int32, shape, dim)


def whole():
    return pl.BlockSpec(memory_space=pltpu.VMEM)


def in_hbm():
    return pl.BlockSpec(memory_space=pltpu.HBM)


def kept(value):
    return pltpu.with_memory_space_constraint(value, pltpu.HBM)


def params(mib):
    return pltpu.CompilerParams(vmem_limit_bytes=mib * MIB)


def fetch(pairs, sems):
    copies = [pltpu.make_async_copy(a, b, sems.at[i]) for i, (a, b) in enumerate(pairs)]
    for copy in copies:
        copy.start()
    for copy in copies:
        copy.wait()


def dot(a, b, dims):
    return lax.dot_general(a, b, (dims, ((), ())), preferred_element_type=F32)


def pack_kernel(
    inner_left_hbm, outer_left_hbm, inner_right_hbm, outer_right_hbm, left_out, right_out,
    inner_left_ref, outer_left_ref, inner_right_ref, outer_right_ref, left_ref, sems
):
    pairs = [
        (inner_left_hbm, inner_left_ref),
        (outer_left_hbm, outer_left_ref),
        (inner_right_hbm, inner_right_ref),
        (outer_right_hbm, outer_right_ref),
    ]
    copies = [pltpu.make_async_copy(a, b, sems.at[i]) for i, (a, b) in enumerate(pairs)]
    for copy in copies:
        copy.start()
    for copy in copies[:2]:
        copy.wait()
    k, lane = iota((16, 128), 0), iota((16, 128), 1)
    inner = jnp.zeros((16, 128), F32)
    for m in range(8):
        pick = (lane == 16 * (k // 2) + 2 * m + k % 2).astype(F32).astype(BF16)
        inner += dot(inner_left_ref[m], pick, ((1,), (0,)))
    k, lane = iota((16, 256), 0), iota((16, 256), 1)
    outer = jnp.zeros((56, 256), F32)
    for l in range(4):
        at = 8 * (k // 2) + 2 * l + k % 2
        pick = jnp.logical_or(lane == at, lane == at + 192).astype(F32).astype(BF16)
        outer += dot(outer_left_ref[l], pick, ((0,), (0,)))
    first, second = outer[:, 0:128], outer[:, 128:256]
    block = jnp.concatenate([inner, first[0:24] + second[24:48], first[48:52] + second[52:56]], axis=0)
    for i in range(left_ref.shape[0]):
        left_ref[i] = block.reshape(11, 4, 128).astype(BF16)
    sent = pltpu.make_async_copy(left_ref, left_out, sems.at[4])
    sent.start()
    for copy in copies[2:]:
        copy.wait()
    row, e = iota((16, 2), 0), iota((16, 2), 1)
    inner = jnp.zeros((16, 448), F32)
    for m in range(8):
        pick = (row == 2 * m + e).astype(F32).astype(BF16)
        inner += dot(pick, inner_right_ref[m], ((1,), (0,)))
    row, e = iota((8, 2), 0), iota((8, 2), 1)
    outer = jnp.zeros((8, 128), F32)
    for l in range(4):
        pick = (row == 2 * l + e).astype(F32).astype(BF16)
        outer += dot(pick, outer_right_ref[l], ((1,), (0,)))
    outer = jnp.concatenate([outer[:, 0:64], outer[:, 64:128]], axis=0)
    right_out[...] = jnp.concatenate([inner, outer], axis=1).astype(BF16)
    sent.wait()


def gather_right_kernel(own_ref, one_ref, two_ref, three_ref, inner_ref, outer_ref, right_ref):
    me = lax.axis_index("row")
    for d, ref in zip((0, *FAR), (own_ref, one_ref, two_ref, three_ref)):
        for core in range(2):
            right_ref[me ^ (d ^ core)] = ref[core].astype(F32)
    inner_ref[...] = right_ref[...].reshape(128, 512).T[0:448, :].astype(BF16)
    ranks = jnp.concatenate([right_ref[:, 0:8, 448:512], right_ref[:, 8:16, 448:512]], axis=2).reshape(64, 128)
    matrix = (iota((64, 128), 0) % 8) // 2
    zero = jnp.zeros((64, 128), F32)
    for l in range(4):
        one = jnp.where(matrix == l, ranks, 0.0)
        outer_ref[l, 0:64, :] = jnp.concatenate([one, zero], axis=1).astype(BF16)
        outer_ref[l, 64:128, :] = jnp.concatenate([zero, one], axis=1).astype(BF16)


def load_kernel(inner_hbm, inner_ref, sems):
    fetch([(inner_hbm.at[0:EARLY], inner_ref)], sems)


def squares_kernel(
    left_ref, inner_right_ref, outer_right_ref, early_ref, inner_hbm, outer_hbm,
    inner_full_ref, outer_full_ref, squares_ref, late_ref, outer_ref, sems
):
    def start_inner(i, carry):
        pltpu.make_async_copy(inner_hbm.at[EARLY + i], late_ref.at[i], sems.at[i]).start()
        return carry

    def start_outer(l, carry):
        pltpu.make_async_copy(outer_hbm.at[l], outer_ref.at[l], sems.at[8 - EARLY + l]).start()
        return carry

    lax.fori_loop(0, 8 - EARLY, start_inner, 0)
    lax.fori_loop(0, 4, start_outer, 0)
    left = left_ref[:, 0:4].astype(F32).reshape(512, 128).astype(BF16)
    matrix = (iota((1, 128), 1) % 16) // 2
    sums = []
    for m in range(8):
        if m == EARLY:
            for i in range(8 - EARLY):
                pltpu.make_async_copy(inner_hbm.at[EARLY + i], late_ref.at[i], sems.at[i]).wait()
        base = early_ref[m] if m < EARLY else late_ref[m - EARLY]
        right = inner_right_ref[...] * (matrix == m).astype(F32).astype(BF16)
        full = base.astype(F32) + dot(right, left, ((1,), (1,)))
        inner_full_ref[m] = full
        square = full * full
        part = (square[:, 0:128] + square[:, 128:256]) + (square[:, 256:384] + square[:, 384:512])
        sums.append(jnp.sum(part.T, axis=0, keepdims=True))
    left = jnp.concatenate([left_ref[:, 4:11], left_ref[:, 10:11]], axis=1).astype(F32)
    left = left.reshape(1024, 128).astype(BF16)
    upper = iota((8, 128), 0) < 4
    tails = []
    for l in range(4):
        pltpu.make_async_copy(outer_hbm.at[l], outer_ref.at[l], sems.at[8 - EARLY + l]).wait()
    for l in range(4):
        delta = dot(left, outer_right_ref[l], ((1,), (0,)))
        total = jnp.zeros((8, 128), F32)
        for c in range(32):
            here = slice(56 * c, 56 * c + 56)
            a, b = delta[32 * c : 32 * c + 32, 0:128], delta[32 * c : 32 * c + 32, 128:256]
            two = jnp.concatenate([a[0:24], b[0:24], jnp.where(upper, a[24:32], b[24:32])], axis=0)
            full = outer_ref[l, here, :].astype(F32) + two
            outer_full_ref[l, here, :] = full
            total += jnp.sum((full * full).reshape(7, 8, 128), axis=0)
        total = jnp.sum(total, axis=0, keepdims=True)
        tails += [total[:, 0:64], total[:, 64:128]]
    squares_ref[...] = jnp.concatenate(
        [jnp.concatenate([s, t], axis=1) for s, t in zip(sums, tails)], axis=0
    )


def scale_kernel(
    own_ref, one_ref, two_ref, three_ref, inner_mag_ref, outer_mag_ref, inner_full_ref, outer_full_ref, inner_out, outer_out, inner_buf, outer_buf, sems
):
    here = lax.axis_index("row")
    scale = lax.rsqrt((own_ref[...] + one_ref[...]) + (two_ref[...] + three_ref[...]) + epsilon)
    mags = jnp.concatenate([inner_mag_ref[i] for i in range(4)], axis=0)
    factor = (scale[:, 0:448] * mags).T

    def sent_outer(l):
        return pltpu.make_async_copy(outer_buf.at[l], outer_out.at[l], sems.at[8 + l])

    def sent_inner(m):
        return pltpu.make_async_copy(inner_buf.at[m], inner_out.at[m], sems.at[m])

    for l in range(4):
        row = jnp.concatenate([scale[2 * l : 2 * l + 1, 448:512], scale[2 * l + 1 : 2 * l + 2, 448:512]], axis=1)
        row = row * outer_mag_ref[l]

        @pl.when(here >= 0)
        def _():
            outer_buf[l] = (outer_full_ref[l] * row).astype(BF16)
            sent_outer(l).start()

    for m in range(8):
        column = factor[:, m : m + 1]

        @pl.when(here >= 0)
        def _():
            inner_buf[m] = (inner_full_ref[m] * column).astype(BF16)
            sent_inner(m).start()

    for l in range(4):
        sent_outer(l).wait()
    for m in range(8):
        sent_inner(m).wait()


def swapped(value, d):
    return lax.ppermute(value, "row", [(i, i ^ d) for i in range(lax.axis_size("row"))])


def shards(
    inner_base, inner_left, inner_right, inner_mag, outer_base, outer_left, outer_right, outer_mag
):
    cols = lax.axis_size("col")
    inner_base = jnp.swapaxes(inner_base, 3, 4).reshape(8, 448, 512)
    outer_base = outer_base.reshape(4, 1792, 128)
    left, right = pl.pallas_call(
        pack_kernel,
        out_shape=(jax.ShapeDtypeStruct((cols, 11, 4, 128), BF16), pltpu.VMEM((16, 512), BF16)),
        in_specs=[in_hbm()] * 4,
        out_specs=(in_hbm(), whole()),
        scratch_shapes=[
            pltpu.VMEM((8, 16, 16), BF16),
            pltpu.VMEM((4, 16, 56), BF16),
            pltpu.VMEM((8, 2, 448), BF16),
            pltpu.VMEM((4, 2, 128), BF16),
            pltpu.VMEM((cols, 11, 4, 128), BF16),
            pltpu.SemaphoreType.DMA((5,)),
        ],
        compiler_params=params(4),
        name="pack",
    )(
        kept(inner_left.reshape(8, 16, 16)),
        kept(jnp.swapaxes(outer_left, 2, 3).reshape(4, 16, 56)),
        kept(inner_right.reshape(8, 2, 448)),
        kept(outer_right.reshape(4, 2, 128)),
    )
    partner = swapped(right, 1)
    left = lax.all_to_all(left, "col", 0, 0, tiled=True)
    right = jnp.stack([right, partner])
    far = [swapped(right, d) for d in FAR]
    early = pl.pallas_call(
        load_kernel,
        out_shape=pltpu.VMEM((EARLY, 448, 512), BF16),
        in_specs=[in_hbm()],
        out_specs=whole(),
        scratch_shapes=[pltpu.SemaphoreType.DMA((1,))],
        compiler_params=params(4),
        name="load",
    )(kept(inner_base))
    inner_ranks, outer_ranks = pl.pallas_call(
        gather_right_kernel,
        out_shape=(pltpu.VMEM((448, 128), BF16), pltpu.VMEM((4, 128, 256), BF16)),
        in_specs=[whole()] * 4,
        out_specs=(whole(), whole()),
        scratch_shapes=[pltpu.VMEM((8, 16, 512), F32)],
        compiler_params=params(4),
        name="gather_right",
    )(right, *far)
    inner_full, outer_full, squares = pl.pallas_call(
        squares_kernel,
        out_shape=(
            pltpu.VMEM((8, 448, 512), F32),
            pltpu.VMEM((4, 1792, 128), F32),
            pltpu.VMEM((8, 512), F32),
        ),
        in_specs=[whole()] * 4 + [in_hbm()] * 2,
        out_specs=(whole(),) * 3,
        scratch_shapes=[
            pltpu.VMEM((8 - EARLY, 448, 512), BF16),
            pltpu.VMEM((4, 1792, 128), BF16),
            pltpu.SemaphoreType.DMA((12 - EARLY,)),
        ],
        compiler_params=params(12),
        name="squares",
    )(left, inner_ranks, outer_ranks, early, kept(inner_base), kept(outer_base))
    squares = squares + swapped(squares, 1)
    far = [swapped(squares, d) for d in FAR]
    inner_merged, outer_merged = pl.pallas_call(
        scale_kernel,
        out_shape=(
            jax.ShapeDtypeStruct((8, 448, 512), BF16),
            jax.ShapeDtypeStruct((4, 1792, 128), BF16),
        ),
        in_specs=[whole()] * 8,
        out_specs=(in_hbm(),) * 2,
        scratch_shapes=[
            pltpu.VMEM((8, 448, 512), BF16),
            pltpu.VMEM((4, 1792, 128), BF16),
            pltpu.SemaphoreType.DMA((12,)),
        ],
        compiler_params=params(12),
        name="scale",
    )(squares, *far, inner_mag.reshape(4, 2, 448), outer_mag, inner_full, outer_full)
    inner_merged = jnp.swapaxes(inner_merged.reshape(4, 1, 2, 448, 512), 3, 4)
    return inner_merged, outer_merged.reshape(4, 1, 1792, 128)


def solution(mesh):
    in_specs = (
        P(None, None, None, "row", "col"),
        P(None, None, None, ("row", "col"), None),
        P(None, None, None, "row", "col"),
        P(None, None, None, "col"),
        P(None, None, "row", "col"),
        P(None, None, ("row", "col"), None),
        P(None, None, "row", "col"),
        P(None, None, "col"),
    )
    out_specs = (P(None, None, None, "row", "col"), P(None, None, "row", "col"))
    return jax.shard_map(shards, mesh=mesh, in_specs=in_specs, out_specs=out_specs, check_vma=False)
```
